32 devices in a mesh: sensor: 4 (over y, x), chan: 8 (over z, core).
Axes of the slice: x: 2, y: 2, z: 4, core: 2. Of those that a mesh axis runs over, the one named last changes fastest.
Arguments:
- samples: float32 [2, 128, 512, 128], P(None, 'sensor', 'chan'), may hold values from -6 to 6
- bins: int32 [64], replicated, may hold values from 1 to 511
- offsets: int32 [64], replicated, may hold values from 0 to 15
Outputs:
- gram: float32 [64, 2, 128, 128], P('chan', None, 'sensor')
The draws below stay inside these ranges and needn't reach their ends.
All inputs are finite; a program needn't handle non-finite values.
Results may differ from the reference program's by a relative error of at most 0.00009.
Values sent between devices are 32-bit elements; how exact they have to be, the bound alone decides.
No kernel may reach another device: no remote copies, remote signals or barrier semaphores. Data moves between devices by JAX's collectives and lax.ppermute only.
A program may use at most 128 MiB of HBM per device.

```python
import math
import jax
import jax.numpy as jnp
from jax import lax

SENSORS = 128
CHANNELS = 128
BLOCKS = 512
ALPHAS = 64
CH_DEV = 16


def plant(values, key, smallest, top_value):
    shape = values.shape
    place = [jax.random.randint(jax.random.fold_in(key, axis), (), 0, shape[axis]) for axis in range(len(shape))]
    values = values.at[tuple(place)].set(smallest)
    longest = shape.index(max(shape))
    place[longest] = (place[longest] + 1) % shape[longest]
    return values.at[tuple(place)].set(top_value)


def shard_levels(rng, dims, split, smallest, largest):
    gain, own = 1.0, jax.random.fold_in(rng, 6)
    for position, blocks in split:
        heights = jnp.exp(jax.random.uniform(jax.random.fold_in(own, position), (blocks,), jnp.float32, smallest / len(split), largest / len(split)))
        gain = gain * jnp.repeat(heights, dims[position] // blocks).reshape([-1 if axis == position else 1 for axis in range(len(dims))])
    return gain


def scatter_about(own_key, shape, deviation, limit, shards=(), kind=jnp.bfloat16):
    level = shard_levels(own_key, shape, shards, -0.22, 0.18) if shards else 1.0
    array = jax.random.normal(own_key, shape, jnp.float32) * deviation * level
    return jnp.minimum(jnp.maximum(array, -limit), limit).astype(kind)


def setup_inputs(seed: int = 0) -> dict:
    seeds = jax.random.split(jax.random.key(seed), 4)
    return {
        "samples": scatter_about(seeds[0], (2, SENSORS, BLOCKS, CHANNELS), 1.0, 6.0, ((1, 4), (2, 8)), jnp.float32),
        "bins": plant(jax.random.randint(seeds[1], (ALPHAS,), 1, BLOCKS), jax.random.fold_in(seeds[1], 1), 1, BLOCKS - 1).astype(jnp.int32),
        "offsets": plant(jax.random.randint(seeds[2], (ALPHAS,), 0, CH_DEV), jax.random.fold_in(seeds[2], 1), 0, CH_DEV - 1).astype(jnp.int32),
    }


power_floor = 0.1

def reference(samples, bins, offsets):
    channel_count = samples.shape[3]
    length = samples.shape[2]
    positions = jnp.arange(channel_count, dtype=jnp.float32)
    window = 0.5 - 0.5 * jnp.cos(positions * (2.0 * math.pi / channel_count))
    signal = samples[0] * window + 1j * (samples[1] * window)
    demodulates = jnp.fft.fft(signal, axis=2) / math.sqrt(channel_count)
    spectra = jnp.fft.fft(demodulates, axis=1) / math.sqrt(length)
    power = jnp.real(spectra) * jnp.real(spectra) + jnp.imag(spectra) * jnp.imag(spectra)
    spectra = spectra / jnp.sqrt(power + power_floor)
    spectra = jnp.transpose(spectra, (0, 2, 1))
    sensors_all = spectra.shape[0]
    flattened = spectra.reshape(sensors_all, -1)
    factor = 1.0 / math.sqrt(channel_count * length)

    def one_alpha(inputs_pair):
        cycle_bin, offset = inputs_pair
        shifted = jnp.roll(spectra, (offset, -cycle_bin), axis=(1, 2)).reshape(sensors_all, -1)
        product = jnp.matmul(shifted, jnp.conj(flattened).T, precision=lax.Precision.HIGHEST) * factor
        return jnp.stack([jnp.real(product), jnp.imag(product)])
    return lax.map(one_alpha, (bins, offsets))
```

```python
import functools
import math

import jax
import jax.numpy as jnp
import ml_dtypes
import numpy as np
from jax import lax
from jax.experimental import pallas as pl
from jax.experimental.pallas import tpu as pltpu
from jax.sharding import PartitionSpec as P

power_floor = 0.1
f32 = jnp.float32
bf16 = jnp.bfloat16
nt_dims = (((1,), (1,)), ((), ()))
nn_dims = (((1,), (0,)), ((), ()))


def halves(table):
    high = table.astype(np.float32).astype(ml_dtypes.bfloat16)
    low = (table - high.astype(np.float64)).astype(ml_dtypes.bfloat16)
    return high, low


def window_table(length):
    index = np.arange(length)
    angles = 2.0 * math.pi / length * (index[:, None] * index[None, :] % length)
    window = 0.5 - 0.5 * np.cos(2.0 * math.pi / length * index)
    scale = window[None, :] / math.sqrt(length)
    high, low = halves(np.concatenate([np.cos(angles) * scale, np.sin(angles) * scale], 1))
    return high.astype(np.float32), low.astype(np.float32)


def block_table(length, pieces):
    index = np.arange(length)
    angles = 2.0 * math.pi / length * (index[:, None] * index[None, :] % length)
    scale = 1.0 / math.sqrt(length)
    pair = [(t * scale).reshape(pieces, length // pieces, length) for t in (np.cos(angles), np.sin(angles))]
    return halves(np.concatenate(pair, 1).reshape(2 * length, length))


def split(value):
    high = value.astype(bf16)
    return high, (value - high.astype(f32)).astype(bf16)


def dot3(left, right, dims):
    lh, ll = left
    rh, rl = right
    dot = functools.partial(lax.dot_general, dimension_numbers=dims, preferred_element_type=f32)
    return dot(lh, rh) + dot(ll, rh) + dot(lh, rl)


def swap(block, axis, distance):
    size = lax.axis_size(axis)
    return lax.ppermute(block, axis, [(i, i ^ distance) for i in range(size)])


def demod_body(ids, samples, table_high, table_low, *outs):
    channels = table_high.shape[0]
    half = outs[0].shape[0]
    chans = 2 * half
    order = [pl.multiple_of(jnp.bitwise_xor(ids[0], r) * chans, chans) for r in range(channels // chans)]
    table = tuple(
        jnp.concatenate([t[pl.ds(start, chans), :] for start in order], 0).astype(bf16) for t in (table_high, table_low)
    )
    for s in range(samples.shape[1]):
        real = samples[0, s]
        imag = samples[1, s]
        upper = jnp.concatenate([real, imag], 1)
        lower = jnp.concatenate([imag, -real], 1)
        framed = jnp.concatenate([upper, lower], 0)
        result = dot3(table, split(framed), nt_dims)
        for i, out in enumerate(outs):
            out[:, s, :] = result[i * half:(i + 1) * half]


def demodulate(ids, samples, peers):
    _, sensors, blocks, channels = samples.shape
    step = min(8, sensors)
    half = channels // peers // 2
    high, low = window_table(channels)
    whole = pl.BlockSpec((channels, 2 * channels), lambda i, *_: (0, 0))
    return pl.pallas_call(
        demod_body,
        grid_spec=pltpu.PrefetchScalarGridSpec(
            num_scalar_prefetch=1,
            grid=(sensors // step,),
            in_specs=[pl.BlockSpec((2, step, blocks, channels), lambda i, *_: (0, i, 0, 0)), whole, whole],
            out_specs=[pl.BlockSpec((half, step, 2 * blocks), lambda i, *_: (0, i, 0))] * (2 * peers),
        ),
        out_shape=[jax.ShapeDtypeStruct((half, sensors, 2 * blocks), f32)] * (2 * peers),
        name="demod",
    )(ids, samples, jnp.asarray(high), jnp.asarray(low))


def spectra_body(ids, *refs, sources, places):
    received = refs[:sources]
    table_high, table_low = refs[sources:sources + 2]
    outs = refs[sources + 2:-4]
    left_high, left_low, right_high, right_low = refs[-4:]
    half, sensors, width = received[0].shape
    rows = half * sensors
    for r in range(sources):
        block = received[r][...].reshape(rows, width)
        turned = jnp.concatenate([block[:, width // 2:], -block[:, :width // 2]], 1)
        place = slice(r * width, (r + 1) * width)
        left_high[:rows, place], left_low[:rows, place] = split(block)
        left_high[rows:, place], left_low[rows:, place] = split(turned)
        start = pl.multiple_of(jnp.bitwise_xor(ids[0], r) * width, width)
        right_high[place, :] = table_high[pl.ds(start, width), :]
        right_low[place, :] = table_low[pl.ds(start, width), :]
    total = dot3((left_high[...], left_low[...]), (right_high[...], right_low[...]), nn_dims)
    real = total[:rows]
    imag = total[rows:]
    scaling = lax.rsqrt(real * real + imag * imag + power_floor)
    for c, part in enumerate((real * scaling, imag * scaling)):
        part = part.reshape(half, sensors, part.shape[1])
        for out, place in zip(outs, places):
            out[:, c] = part[place]


def whitened(ids, received, pieces):
    sources = len(received)
    half, sensors, width = received[0].shape
    length = sources * width // 2
    rows = 2 * half * sensors
    high, low = block_table(length, sources)
    shapes = [jax.ShapeDtypeStruct((half, 2, sensors, length), f32)]
    places = [slice(0, half)]
    for i in range(pieces):
        shapes.append(jax.ShapeDtypeStruct((half // pieces, 2, sensors, length), f32))
        places.append(slice(i * half // pieces, (i + 1) * half // pieces))
    return pl.pallas_call(
        functools.partial(spectra_body, sources=sources, places=places),
        grid_spec=pltpu.PrefetchScalarGridSpec(
            num_scalar_prefetch=1,
            grid=(1,),
            in_specs=[pl.BlockSpec((half, sensors, width), lambda i, *_: (0, 0, 0))] * sources
            + [pl.BlockSpec((2 * length, length), lambda i, *_: (0, 0))] * 2,
            out_specs=[pl.BlockSpec(shape.shape, lambda i, *_: (0, 0, 0, 0)) for shape in shapes],
            scratch_shapes=[pltpu.VMEM((rows, 2 * length), bf16)] * 2 + [pltpu.VMEM((2 * length, length), bf16)] * 2,
        ),
        out_shape=shapes,
        cost_estimate=pl.CostEstimate(
            flops=12 * rows * length * length, transcendentals=0, bytes_accessed=8 << 20
        ),
        name="spectra",
    )(ids, *received, jnp.asarray(high), jnp.asarray(low))


def gram_body(ids, bins, offsets, *refs, spans, parts, peers, devices, base, final, factor, group):
    window, refs = refs[:spans], refs[spans:]
    columns = [refs[parts * g:parts * (g + 1)] for g in range(peers)]
    refs = refs[parts * peers:]
    if final:
        before, refs = refs[0], refs[1:]
    outs, refs = (refs[:2], refs[2:]) if final else (refs[:1], refs[1:])
    extended, fresh, left_high, left_low, right_high, right_low, sums, sems, fresh_sems = refs[:9]
    k = pl.program_id(0)
    steps = pl.num_programs(0)
    size = columns[0][0].shape[0]
    sensors, length = window[0].shape[2:]
    rows = 2 * sensors
    alphas = sums.shape[0] // rows
    tiles = length // 128
    blocks = alphas // group
    each = bins.shape[0] // (2 * devices)
    here = each * devices

    def arrivals(chan, part):
        slot = lax.rem(chan, 2)
        return [
            pltpu.make_async_copy(columns[g][part].at[lax.rem(chan, size)], fresh.at[slot, g], fresh_sems.at[slot, g])
            for g in range(peers)
        ]

    def request(chan):
        for part in range(parts):

            @pl.when((chan >= part * size) & (chan < (part + 1) * size))
            def _():
                for copy in arrivals(chan, part):
                    copy.start()

    def pieces():
        copies = []
        start = 0
        for i, part in enumerate(window):
            copies.append(pltpu.make_async_copy(part, extended.at[start:start + part.shape[0]], sems.at[i]))
            start += part.shape[0]
        if final:
            copies.append(pltpu.make_async_copy(before.at[base:base + alphas], refs[9], sems.at[spans]))
        return copies

    @pl.when(k == 0)
    def _():
        request(k)
        for copy in pieces():
            copy.start()
        sums[...] = jnp.zeros(sums.shape, f32)

    for copy in arrivals(k, 0):
        copy.wait()
    request(k + 1)

    slot = lax.rem(k, 2)
    for g in range(peers):
        peer = jnp.bitwise_xor(ids[1], g)
        for c in range(2):
            high, low = split(fresh[slot, g, c])
            place = pl.ds(pl.multiple_of((c * peers + peer) * sensors, sensors), sensors)
            for t in range(tiles):
                right_high[t, place] = high[:, t * 128:(t + 1) * 128]
                right_low[t, place] = low[:, t * 128:(t + 1) * 128]

    lane = lax.broadcasted_iota(jnp.int32, (rows, 128), 1)

    def build(chan, block, slot):
        for a in range(group):
            whole = base + block * group + a
            position = lax.rem(whole, here)
            lane_group = position // each
            device = 2 * lax.rem(lane_group, devices // 2) + lane_group // (devices // 2)
            j = jnp.bitwise_xor(ids[0], device) * (2 * each) + (whole // here) * each + lax.rem(position, each)
            q = bins[j]
            source = chan + 2 * steps - offsets[j]
            tile = lax.shift_right_logical(q, 7)
            rest = jnp.bitwise_and(q, 127)
            turn = jnp.bitwise_and(128 - rest, 127)
            keep = lane < 128 - rest
            turned = []
            for t in range(tiles):
                start = pl.multiple_of(lax.rem(tile + t, tiles) * 128, 128)
                data = extended[source, :, :, pl.ds(start, 128)].reshape(rows, 128)
                turned.append(pltpu.roll(data, turn, 1))
            for t in range(tiles):
                high, low = split(jnp.where(keep, turned[t], turned[(t + 1) % tiles]))
                left_high[slot, t, a * rows:(a + 1) * rows] = high
                left_low[slot, t, a * rows:(a + 1) * rows] = low

    def joined(ref):
        return jnp.concatenate([ref[t] for t in range(tiles)], 1)

    def multiply(block, slot):
        place = pl.ds(pl.multiple_of(block * (group * rows), group * rows), group * rows)
        left = (joined(left_high.at[slot]), joined(left_low.at[slot]))
        product = dot3(left, (joined(right_high), joined(right_low)), nt_dims)
        sums[place] = sums[place] + product

    @pl.when(k == 0)
    def _():
        for copy in pieces()[:spans]:
            copy.wait()
        build(0, 0, 0)

    def pair(i, carry):
        build(k, 2 * i + 1, 1)
        multiply(2 * i, 0)
        wrap = 2 * i + 2 == blocks
        build(jnp.where(wrap, jnp.minimum(k + 1, steps - 1), k), jnp.where(wrap, 0, 2 * i + 2), 0)
        multiply(2 * i + 1, 1)
        return carry

    lax.fori_loop(0, blocks // 2, pair, 0)

    @pl.when(k == steps - 1)
    def _():
        count = outs[0].shape[3]
        extent = outs[0].shape[0]
        if final:
            pieces()[spans].wait()

        for piece, out in enumerate(outs):

            def finish(j, carry):
                position = piece * extent + j
                cross = sums[pl.ds(pl.multiple_of(position * rows, rows), rows)]
                real = cross[:sensors, :count] + cross[sensors:, count:]
                imag = cross[sensors:, :count] - cross[:sensors, count:]
                if final:
                    real = (real + refs[9][position, 0]) * factor
                    imag = (imag + refs[9][position, 1]) * factor
                out[j, 0] = real
                out[j, 1] = imag
                return carry

            lax.fori_loop(0, extent, finish, 0, unroll=4)


def gram_sums(ids, bins, offsets, window, columns, before, side, devices, factor):
    half, _, sensors, length = window[0].shape
    peers = len(columns)
    parts = len(columns[0])
    spans = len(window)
    final = before is not None
    outs = 2 if final else 1
    alphas = bins.shape[0] // outs
    count = peers * sensors
    rows = 2 * sensors
    group = min(alphas // 2, 512 // rows)
    anywhere = pl.BlockSpec(memory_space=pl.ANY)
    tiles = length // 128
    shape = (alphas // outs, 2, sensors, count)
    return pl.pallas_call(
        functools.partial(
            gram_body, spans=spans, parts=parts, peers=peers, devices=devices, base=side * alphas, final=final, factor=factor, group=group
        ),
        grid_spec=pltpu.PrefetchScalarGridSpec(
            num_scalar_prefetch=3,
            grid=(half,),
            in_specs=[anywhere] * (spans + parts * peers + outs - 1),
            out_specs=[pl.BlockSpec(shape, lambda k, *_: (0, 0, 0, 0))] * outs,
            scratch_shapes=[
                pltpu.VMEM((3 * half, 2, sensors, length), f32),
                pltpu.VMEM((2, peers, 2, sensors, length), f32),
                pltpu.VMEM((2, tiles, group * rows, 128), bf16),
                pltpu.VMEM((2, tiles, group * rows, 128), bf16),
                pltpu.VMEM((tiles, 2 * count, 128), bf16),
                pltpu.VMEM((tiles, 2 * count, 128), bf16),
                pltpu.VMEM((alphas * rows, 2 * count), f32),
                pltpu.SemaphoreType.DMA((spans + 1,)),
                pltpu.SemaphoreType.DMA((2, peers)),
            ]
            + [pltpu.VMEM((alphas, 2, sensors, count), f32)] * (outs - 1),
        ),
        out_shape=[jax.ShapeDtypeStruct(shape, f32)] * outs,
        cost_estimate=pl.CostEstimate(
            flops=6 * half * length * alphas * rows * 2 * count, transcendentals=0, bytes_accessed=8 << 20
        ),
        name="gram",
    )(ids, bins, offsets, *window, *[part for group in columns for part in group], *([before] if final else []))


def on_device(samples, bins, offsets):
    chan_count = lax.axis_size("chan")
    peers = lax.axis_size("sensor")
    channels = samples.shape[3]
    ids = jnp.stack([lax.axis_index("chan"), lax.axis_index("sensor")]).astype(jnp.int32)
    pieces = demodulate(ids, samples, chan_count)
    received = [None, None]
    for side in (1, 0):
        received[side] = [pieces[side]] + [None] * (chan_count - 1)
        for r in range(1, chan_count):
            received[side][r] = swap(pieces[2 * r + side], "chan", r)
    route = [(i, (i + 1) % chan_count) for i in range(chan_count)]
    upper_whole, *uppers = whitened(ids, received[1], 2)
    upper_rim = lax.ppermute(upper_whole, "chan", route)
    columns = [{0: part} for part in uppers]
    single = [r for r in range(1, peers) if r & (r - 1) == 0]
    for i, gathered in enumerate(columns):
        for r in single if i else single[::-1]:
            gathered[r] = swap(gathered[0], "sensor", r)
    for i, gathered in enumerate(columns):
        for r in range(1, peers):
            if r not in single:
                bits = [b for b in single if r & b]
                bit = bits[0] if i else bits[-1]
                gathered[r] = swap(gathered[r ^ bit], "sensor", bit)
    upper_columns = [[gathered[r] for gathered in columns] for r in range(peers)]
    (lower,) = whitened(ids, received[0], 0)
    lower_columns = [[lower]] + [[swap(lower, "sensor", r)] for r in range(1, peers)]
    lower_rim = lax.ppermute(lower, "chan", route)
    length = lower.shape[3]
    factor = 1.0 / math.sqrt(channels * length)
    upper_window = [upper_rim, lower] + uppers
    lower_window = [lower_rim, upper_rim, lower]
    scan = functools.partial(gram_sums, ids, bins, offsets, devices=chan_count, factor=factor)
    upper = scan(upper_window, upper_columns, None, 0)[0]
    results = []
    for side in range(2):
        same, other = scan(lower_window, lower_columns, upper, side)
        near = swap(other, "chan", 1)
        each = same.shape[0] // (chan_count // 2)
        total = None
        for q in range(chan_count // 2 - 1, -1, -1):
            place = slice(q * each, (q + 1) * each)
            both = same[place] + near[place]
            if q:
                both = swap(both, "chan", 2 * q)
            total = both if total is None else total + both
        results.append(total)
    return jnp.concatenate(results, 0)


def solution(mesh):
    return jax.shard_map(
        on_device,
        mesh=mesh,
        in_specs=(P(None, "sensor", "chan", None), P(), P()),
        out_specs=P("chan", None, "sensor", None),
        check_vma=False,
    )
```

```python
import functools
import math

import jax
import jax.numpy as jnp
import ml_dtypes
import numpy as np
from jax import lax
from jax.experimental import pallas as pl
from jax.experimental.pallas import tpu as pltpu
from jax.sharding import PartitionSpec as P

power_floor = 0.1
f32 = jnp.float32
bf16 = jnp.bfloat16
nt_dims = (((1,), (1,)), ((), ()))
nn_dims = (((1,), (0,)), ((), ()))


def halves(table):
    high = table.astype(np.float32).astype(ml_dtypes.bfloat16)
    low = (table - high.astype(np.float64)).astype(ml_dtypes.bfloat16)
    return high, low


def window_table(length):
    index = np.arange(length)
    angles = 2.0 * math.pi / length * (index[:, None] * index[None, :] % length)
    window = 0.5 - 0.5 * np.cos(2.0 * math.pi / length * index)
    scale = window[None, :] / math.sqrt(length)
    high, low = halves(np.concatenate([np.cos(angles) * scale, np.sin(angles) * scale], 1))
    return high, low


def block_table(length, pieces):
    index = np.arange(length)
    angles = 2.0 * math.pi / length * (index[:, None] * index[None, :] % length)
    scale = 1.0 / math.sqrt(length)
    pair = [(t * scale).reshape(pieces, length // pieces, length) for t in (np.cos(angles), np.sin(angles))]
    return halves(np.concatenate(pair, 1).reshape(2 * length, length))


def split(value):
    high = value.astype(bf16)
    return high, (value - high.astype(f32)).astype(bf16)


def dot3(left, right, dims):
    lh, ll = left
    rh, rl = right
    dot = functools.partial(lax.dot_general, dimension_numbers=dims, preferred_element_type=f32)
    return dot(lh, rh) + dot(ll, rh) + dot(lh, rl)


def swap(block, axis, distance):
    size = lax.axis_size(axis)
    return lax.ppermute(block, axis, [(i, i ^ distance) for i in range(size)])


def demod_body(samples, table_high, table_low, *outs):
    table = (table_high[...], table_low[...])
    devices, half = outs[0].shape[:2]
    for s in range(samples.shape[1]):
        real = samples[0, s]
        imag = samples[1, s]
        upper = jnp.concatenate([real, imag], 1)
        lower = jnp.concatenate([imag, -real], 1)
        framed = jnp.concatenate([upper, lower], 0)
        result = dot3(table, split(framed), nt_dims)
        for device in range(devices):
            for side, out in enumerate(outs):
                start = (2 * device + side) * half
                out[device, :, s, :] = result[start:start + half]


def demodulate(samples, devices):
    _, sensors, blocks, channels = samples.shape
    step = min(8, sensors)
    half = channels // devices // 2
    high, low = window_table(channels)
    whole = pl.BlockSpec((channels, 2 * channels), lambda i: (0, 0))
    return pl.pallas_call(
        demod_body,
        grid=(sensors // step,),
        in_specs=[pl.BlockSpec((2, step, blocks, channels), lambda i: (0, i, 0, 0)), whole, whole],
        out_specs=[pl.BlockSpec((devices, half, step, 2 * blocks), lambda i: (0, 0, i, 0))] * 2,
        out_shape=[jax.ShapeDtypeStruct((devices, half, sensors, 2 * blocks), f32)] * 2,
        name="demod",
    )(samples, jnp.asarray(high), jnp.asarray(low))


def spectra_body(received, table_high, table_low, *refs, places):
    outs = refs[:-2]
    left_high, left_low = refs[-2:]
    sources, half, sensors, width = received.shape
    rows = half * sensors
    for p in range(sources):
        block = received[p].reshape(rows, width)
        turned = jnp.concatenate([block[:, width // 2:], -block[:, :width // 2]], 1)
        place = slice(p * width, (p + 1) * width)
        left_high[:rows, place], left_low[:rows, place] = split(block)
        left_high[rows:, place], left_low[rows:, place] = split(turned)
    total = dot3((left_high[...], left_low[...]), (table_high[...], table_low[...]), nn_dims)
    real = total[:rows]
    imag = total[rows:]
    scaling = lax.rsqrt(real * real + imag * imag + power_floor)
    for c, part in enumerate((real * scaling, imag * scaling)):
        part = part.reshape(half, sensors, part.shape[1])
        for t in range(part.shape[2] // 128):
            for out, place in zip(outs, places):
                out[:, t, c] = part[place, :, t * 128:(t + 1) * 128]


def whitened(received, pieces):
    sources, half, sensors, width = received.shape
    length = sources * width // 2
    rows = 2 * half * sensors
    high, low = block_table(length, sources)
    tiles = length // 128
    shapes = [jax.ShapeDtypeStruct((half, tiles, 2, sensors, 128), f32)]
    places = [slice(0, half)]
    for i in range(pieces):
        shapes.append(jax.ShapeDtypeStruct((half // pieces, tiles, 2, sensors, 128), f32))
        places.append(slice(i * half // pieces, (i + 1) * half // pieces))
    return pl.pallas_call(
        functools.partial(spectra_body, places=places),
        scratch_shapes=[pltpu.VMEM((rows, 2 * length), bf16)] * 2,
        out_shape=shapes,
        cost_estimate=pl.CostEstimate(
            flops=12 * rows * length * length, transcendentals=0, bytes_accessed=8 << 20
        ),
        name="spectra",
    )(received, jnp.asarray(high), jnp.asarray(low))


def gram_body(ids, bins, offsets, *refs, spans, parts, peers, devices, turns, turn, final, factor, group):
    window, refs = refs[:spans], refs[spans:]
    columns = [refs[parts * g:parts * (g + 1)] for g in range(peers)]
    refs = refs[parts * peers:]
    if final:
        before, refs = refs[0], refs[1:]
    outs, refs = (refs[:2], refs[2:]) if final else (refs[:1], refs[1:])
    extended, fresh, left_high, left_low, right_high, right_low, sums, plan, sems, fresh_sems = refs[:10]
    k = pl.program_id(0)
    steps = pl.num_programs(0)
    size = columns[0][0].shape[0]
    tiles, _, sensors, _ = window[0].shape[1:]
    rows = 2 * sensors
    alphas = sums.shape[0] // rows
    blocks = alphas // group
    starts = [sum(turns[:i]) for i in range(len(turns))]
    base = starts[turn] * devices

    def arrivals(chan, part):
        slot = lax.rem(chan, 2)
        return [
            pltpu.make_async_copy(columns[g][part].at[lax.rem(chan, size)], fresh.at[slot, g], fresh_sems.at[slot, g])
            for g in range(peers)
        ]

    def request(chan):
        for part in range(parts):

            @pl.when((chan >= part * size) & (chan < (part + 1) * size))
            def _():
                for copy in arrivals(chan, part):
                    copy.start()

    def pieces():
        copies = []
        start = 0
        for i, part in enumerate(window):
            copies.append(pltpu.make_async_copy(part, extended.at[start:start + part.shape[0]], sems.at[i]))
            start += part.shape[0]
        if final:
            copies.append(pltpu.make_async_copy(before.at[base:base + alphas], refs[10], sems.at[spans]))
        return copies

    @pl.when(k == 0)
    def _():
        request(k)
        for copy in pieces():
            copy.start()
        sums[...] = jnp.zeros(sums.shape, f32)

    for copy in arrivals(k, 0):
        copy.wait()
    request(k + 1)

    slot = lax.rem(k, 2)
    for g in range(peers):
        peer = jnp.bitwise_xor(ids[1], g)
        for c in range(2):
            place = pl.ds(pl.multiple_of((c * peers + peer) * sensors, sensors), sensors)
            for t in range(tiles):
                right_high[t, place], right_low[t, place] = split(fresh[slot, g, t, c])

    lane = lax.broadcasted_iota(jnp.int32, (rows, 128), 1)

    def build(chan, block, slot):
        for a in range(group):
            index = block * group + a
            source = chan + plan[0, index]
            tile = plan[1, index]
            rest = plan[2, index]
            turn = jnp.bitwise_and(128 - rest, 127)
            keep = lane < 128 - rest
            turned = []
            for t in range(tiles):
                data = extended[source, jnp.bitwise_and(tile + t, tiles - 1)].reshape(rows, 128)
                turned.append(pltpu.roll(data, turn, 1))
            for t in range(tiles):
                high, low = split(jnp.where(keep, turned[t], turned[(t + 1) % tiles]))
                left_high[slot, t, a * rows:(a + 1) * rows] = high
                left_low[slot, t, a * rows:(a + 1) * rows] = low

    def prepare(i, carry):
        position = base + i
        each, start = jnp.int32(turns[0]), jnp.int32(starts[0])
        for more, place in zip(turns[1:], starts[1:]):
            each = jnp.where(position < place * devices, each, more)
            start = jnp.where(position < place * devices, start, place)
        position = position - start * devices
        lane_group = position // each
        device = 2 * lax.rem(lane_group, devices // 2) + lane_group // (devices // 2)
        j = jnp.bitwise_xor(ids[0], device) * sum(turns) + start + lax.rem(position, each)
        q = bins[j]
        plan[0, i] = 2 * steps - offsets[j]
        plan[1, i] = lax.shift_right_logical(q, 7)
        plan[2, i] = jnp.bitwise_and(q, 127)
        return carry

    def joined(ref, extent):
        return jnp.concatenate([ref[t, :extent] for t in range(tiles)], 1)

    def multiply(block, slot):
        place = pl.ds(pl.multiple_of(block * (group * rows), group * rows), group * rows)
        left = (joined(left_high.at[slot], group * rows), joined(left_low.at[slot], group * rows))
        count = sums.shape[1]
        product = dot3(left, (joined(right_high, count), joined(right_low, count)), nt_dims)
        sums[place] = sums[place] + product

    @pl.when(k == 0)
    def _():
        lax.fori_loop(0, alphas, prepare, 0)
        for copy in pieces()[:spans]:
            copy.wait()
        build(0, 0, 0)

    def pair(i, carry):
        build(k, 2 * i + 1, 1)
        multiply(2 * i, 0)
        wrap = 2 * i + 2 == blocks
        build(jnp.where(wrap, jnp.minimum(k + 1, steps - 1), k), jnp.where(wrap, 0, 2 * i + 2), 0)
        multiply(2 * i + 1, 1)
        return carry

    lax.fori_loop(0, blocks // 2, pair, 0)

    @pl.when(k == steps - 1)
    def _():
        count = outs[0].shape[3]
        extent = outs[0].shape[0]
        if final:
            pieces()[spans].wait()

        for piece, out in enumerate(outs):

            def finish(j, carry):
                position = piece * extent + j
                cross = sums[pl.ds(pl.multiple_of(position * rows, rows), rows)]
                real = cross[:sensors, :count] + cross[sensors:, count:]
                imag = cross[sensors:, :count] - cross[:sensors, count:]
                if final:
                    real = (real + refs[10][position, 0]) * factor
                    imag = (imag + refs[10][position, 1]) * factor
                out[j, 0] = real
                out[j, 1] = imag
                return carry

            lax.fori_loop(0, extent, finish, 0, unroll=4)


def gram_sums(ids, bins, offsets, window, columns, before, turns, turn, devices, factor):
    half, tiles, _, sensors, _ = window[0].shape
    peers = len(columns)
    parts = len(columns[0])
    spans = len(window)
    final = before is not None
    outs = 2 if final else 1
    alphas = turns[turn] * devices if final else bins.shape[0]
    count = peers * sensors
    rows = 2 * sensors
    group = max(g for g in range(1, 1024 // rows + 1) if alphas % (2 * g) == 0)
    anywhere = pl.BlockSpec(memory_space=pl.ANY)
    shape = (alphas // outs, 2, sensors, count)
    return pl.pallas_call(
        functools.partial(
            gram_body, spans=spans, parts=parts, peers=peers, devices=devices, turns=turns, turn=turn, final=final, factor=factor, group=group
        ),
        grid_spec=pltpu.PrefetchScalarGridSpec(
            num_scalar_prefetch=3,
            grid=(half,),
            in_specs=[anywhere] * (spans + parts * peers + outs - 1),
            out_specs=[pl.BlockSpec(shape, lambda k, *_: (0, 0, 0, 0))] * outs,
            scratch_shapes=[
                pltpu.VMEM((3 * half, tiles, 2, sensors, 128), f32),
                pltpu.VMEM((2, peers, tiles, 2, sensors, 128), f32),
                pltpu.VMEM((2, tiles, group * rows + 16, 128), bf16),
                pltpu.VMEM((2, tiles, group * rows + 16, 128), bf16),
                pltpu.VMEM((tiles, 2 * count + 16, 128), bf16),
                pltpu.VMEM((tiles, 2 * count + 16, 128), bf16),
                pltpu.VMEM((alphas * rows, 2 * count), f32),
                pltpu.SMEM((3, alphas), jnp.int32),
                pltpu.SemaphoreType.DMA((spans + 1,)),
                pltpu.SemaphoreType.DMA((2, peers)),
            ]
            + [pltpu.VMEM((alphas, 2, sensors, count), f32)] * (outs - 1),
        ),
        out_shape=[jax.ShapeDtypeStruct(shape, f32)] * outs,
        cost_estimate=pl.CostEstimate(
            flops=6 * half * tiles * 128 * alphas * rows * 2 * count, transcendentals=0, bytes_accessed=8 << 20
        ),
        name="gram",
    )(ids, bins, offsets, *window, *[part for group in columns for part in group], *([before] if final else []))


def on_device(samples, bins, offsets):
    chan_count = lax.axis_size("chan")
    peers = lax.axis_size("sensor")
    channels = samples.shape[3]
    ids = jnp.stack([lax.axis_index("chan"), lax.axis_index("sensor")]).astype(jnp.int32)
    pieces = demodulate(samples, chan_count)
    received = []
    for side in range(2):
        received.append(lax.all_to_all(pieces[side], "chan", split_axis=0, concat_axis=0, tiled=True))
    route = [(i, (i + 1) % chan_count) for i in range(chan_count)]
    upper_whole, *uppers = whitened(received[1], 2)
    upper_rim = lax.ppermute(upper_whole, "chan", route)
    columns = [{0: part} for part in uppers]
    single = [r for r in range(1, peers) if r & (r - 1) == 0]
    for i, gathered in enumerate(columns):
        for r in single if i else single[::-1]:
            gathered[r] = swap(gathered[0], "sensor", r)
    for i, gathered in enumerate(columns):
        for r in range(1, peers):
            if r not in single:
                bits = [b for b in single if r & b]
                bit = bits[0] if i else bits[-1]
                gathered[r] = swap(gathered[r ^ bit], "sensor", bit)
    upper_columns = [[gathered[r] for gathered in columns] for r in range(peers)]
    (lower,) = whitened(received[0], 0)
    lower_columns = [[lower]] + [[swap(lower, "sensor", r)] for r in range(1, peers)]
    lower_rim = lax.ppermute(lower, "chan", route)
    factor = 1.0 / math.sqrt(channels * samples.shape[2] * chan_count)
    share = bins.shape[0] // chan_count
    turns = (share - share // 4, share // 4)
    upper_window = [upper_rim, lower] + uppers
    lower_window = [lower_rim, upper_rim, lower]
    scan = functools.partial(gram_sums, ids, bins, offsets, devices=chan_count, factor=factor)
    upper = scan(upper_window, upper_columns, None, turns, 0)[0]
    results = []
    for side in range(2):
        same, other = scan(lower_window, lower_columns, upper, turns, side)
        near = swap(other, "chan", 1)
        each = same.shape[0] // (chan_count // 2)
        total = None
        for q in range(chan_count // 2 - 1, -1, -1):
            place = slice(q * each, (q + 1) * each)
            both = same[place] + near[place]
            if q:
                both = swap(both, "chan", 2 * q)
            total = both if total is None else total + both
        results.append(total)
    return jnp.concatenate(results, 0)


def solution(mesh):
    return jax.shard_map(
        on_device,
        mesh=mesh,
        in_specs=(P(None, "sensor", "chan", None), P(), P()),
        out_specs=P("chan", None, "sensor", None),
        check_vma=False,
    )
```

```python
import functools
import math

import jax
import jax.numpy as jnp
import ml_dtypes
import numpy as np
from jax import lax
from jax.experimental import pallas as pl
from jax.experimental.pallas import tpu as pltpu
from jax.sharding import PartitionSpec as P

power_floor = 0.1
f32 = jnp.float32
bf16 = jnp.bfloat16
nt_dims = (((1,), (1,)), ((), ()))
nn_dims = (((1,), (0,)), ((), ()))


def halves(table):
    high = table.astype(np.float32).astype(ml_dtypes.bfloat16)
    low = (table - high.astype(np.float64)).astype(ml_dtypes.bfloat16)
    return high, low


def window_table(length):
    index = np.arange(length)
    angles = 2.0 * math.pi / length * (index[:, None] * index[None, :] % length)
    window = 0.5 - 0.5 * np.cos(2.0 * math.pi / length * index)
    scale = window[None, :] / math.sqrt(length)
    high, low = halves(np.concatenate([np.cos(angles) * scale, np.sin(angles) * scale], 1))
    return high, low


def block_table(length, pieces):
    index = np.arange(length)
    angles = 2.0 * math.pi / length * (index[:, None] * index[None, :] % length)
    scale = 1.0 / math.sqrt(length)
    pair = [(t * scale).reshape(pieces, length // pieces, length) for t in (np.cos(angles), np.sin(angles))]
    return halves(np.concatenate(pair, 1).reshape(2 * length, length))


def split(value):
    high = value.astype(bf16)
    return high, (value - high.astype(f32)).astype(bf16)


def dot3(left, right, dims):
    lh, ll = left
    rh, rl = right
    dot = functools.partial(lax.dot_general, dimension_numbers=dims, preferred_element_type=f32)
    return dot(lh, rh) + dot(ll, rh) + dot(lh, rl)


def swap(block, axis, distance):
    size = lax.axis_size(axis)
    return lax.ppermute(block, axis, [(i, i ^ distance) for i in range(size)])


def demod_body(samples, table_high, table_low, *outs):
    table = (table_high[...], table_low[...])
    devices, half = outs[0].shape[:2]
    for s in range(samples.shape[1]):
        real = samples[0, s]
        imag = samples[1, s]
        upper = jnp.concatenate([real, imag], 1)
        lower = jnp.concatenate([imag, -real], 1)
        framed = jnp.concatenate([upper, lower], 0)
        result = dot3(table, split(framed), nt_dims)
        for device in range(devices):
            for side, out in enumerate(outs):
                start = (2 * device + side) * half
                out[device, :, s, :] = result[start:start + half]


def demodulate(samples, devices):
    _, sensors, blocks, channels = samples.shape
    step = min(8, sensors)
    half = channels // devices // 2
    high, low = window_table(channels)
    whole = pl.BlockSpec((channels, 2 * channels), lambda i: (0, 0))
    return pl.pallas_call(
        demod_body,
        grid=(sensors // step,),
        in_specs=[pl.BlockSpec((2, step, blocks, channels), lambda i: (0, i, 0, 0)), whole, whole],
        out_specs=[pl.BlockSpec((devices, half, step, 2 * blocks), lambda i: (0, 0, i, 0))] * 2,
        out_shape=[jax.ShapeDtypeStruct((devices, half, sensors, 2 * blocks), f32)] * 2,
        name="demod",
    )(samples, jnp.asarray(high), jnp.asarray(low))


def spectra_body(received, table_high, table_low, *refs, places):
    outs = refs[:-3]
    left_high, left_low, sums = refs[-3:]
    sources, half, sensors, width = received.shape
    rows = half * sensors
    for p in range(sources):
        block = received[p].reshape(rows, width)
        turned = jnp.concatenate([block[:, width // 2:], -block[:, :width // 2]], 1)
        place = slice(p * width, (p + 1) * width)
        left_high[:rows, place], left_low[:rows, place] = split(block)
        left_high[rows:, place], left_low[rows:, place] = split(turned)
    product = dot3((left_high[...], left_low[...]), (table_high[...], table_low[...]), nn_dims)

    @pl.when(pl.program_id(0) == 0)
    def _():
        sums[...] = product

    @pl.when(pl.program_id(0) == 1)
    def _():
        total = sums[...] + product
        real = total[:rows]
        imag = total[rows:]
        scaling = lax.rsqrt(real * real + imag * imag + power_floor)
        for c, part in enumerate((real * scaling, imag * scaling)):
            part = part.reshape(half, sensors, part.shape[1])
            for t in range(part.shape[2] // 128):
                for out, place in zip(outs, places):
                    out[:, t, c] = part[place, :, t * 128:(t + 1) * 128]


def whitened(received, pieces):
    sources, half, sensors, width = received.shape
    length = sources * width // 2
    rows = 2 * half * sensors
    high, low = block_table(length, sources)
    tiles = length // 128
    shapes = [jax.ShapeDtypeStruct((half, tiles, 2, sensors, 128), f32)]
    places = [slice(0, half)]
    for i in range(pieces):
        shapes.append(jax.ShapeDtypeStruct((half // pieces, tiles, 2, sensors, 128), f32))
        places.append(slice(i * half // pieces, (i + 1) * half // pieces))
    return pl.pallas_call(
        functools.partial(spectra_body, places=places),
        grid=(2,),
        in_specs=[pl.BlockSpec((sources // 2, half, sensors, width), lambda i: (i, 0, 0, 0))]
        + [pl.BlockSpec((length, length), lambda i: (i, 0))] * 2,
        out_specs=[pl.BlockSpec(shape.shape, lambda i: (0, 0, 0, 0, 0)) for shape in shapes],
        scratch_shapes=[pltpu.VMEM((rows, length), bf16)] * 2 + [pltpu.VMEM((rows, length), f32)],
        out_shape=shapes,
        cost_estimate=pl.CostEstimate(
            flops=12 * rows * length * length, transcendentals=0, bytes_accessed=8 << 20
        ),
        name="spectra",
    )(received, jnp.asarray(high), jnp.asarray(low))


def gram_body(ids, bins, offsets, *refs, spans, parts, peers, devices, turns, turn, final, factor, group):
    window, refs = refs[:spans], refs[spans:]
    columns = [refs[parts * g:parts * (g + 1)] for g in range(peers)]
    refs = refs[parts * peers:]
    if final:
        before, refs = refs[0], refs[1:]
    outs, refs = (refs[:2], refs[2:]) if final else (refs[:1], refs[1:])
    extended, fresh, left_high, left_low, right_high, right_low, sums, plan, sems, fresh_sems = refs[:10]
    k = pl.program_id(0)
    steps = pl.num_programs(0)
    size = columns[0][0].shape[0]
    tiles, _, sensors, _ = window[0].shape[1:]
    rows = 2 * sensors
    alphas = sums.shape[0] // rows
    blocks = alphas // group
    starts = [sum(turns[:i]) for i in range(len(turns))]
    base = starts[turn] * devices

    def arrivals(chan, part):
        slot = lax.rem(chan, 2)
        return [
            pltpu.make_async_copy(columns[g][part].at[lax.rem(chan, size)], fresh.at[slot, g], fresh_sems.at[slot, g])
            for g in range(peers)
        ]

    def request(chan):
        for part in range(parts):

            @pl.when((chan >= part * size) & (chan < (part + 1) * size))
            def _():
                for copy in arrivals(chan, part):
                    copy.start()

    def pieces():
        copies = []
        start = 0
        for i, part in enumerate(window):
            copies.append(pltpu.make_async_copy(part, extended.at[start:start + part.shape[0]], sems.at[i]))
            start += part.shape[0]
        if final:
            copies.append(pltpu.make_async_copy(before.at[base:base + alphas], refs[10], sems.at[spans]))
        return copies

    @pl.when(k == 0)
    def _():
        request(k)
        for copy in pieces():
            copy.start()
        sums[...] = jnp.zeros(sums.shape, f32)

    for copy in arrivals(k, 0):
        copy.wait()
    request(k + 1)

    slot = lax.rem(k, 2)
    for g in range(peers):
        peer = jnp.bitwise_xor(ids[1], g)
        for c in range(2):
            place = pl.ds(pl.multiple_of((c * peers + peer) * sensors, sensors), sensors)
            for t in range(tiles):
                right_high[t, place], right_low[t, place] = split(fresh[slot, g, t, c])

    lane = lax.broadcasted_iota(jnp.int32, (rows, 128), 1)

    def build(chan, block, slot):
        for a in range(group):
            index = block * group + a
            source = chan + plan[0, index]
            tile = plan[1, index]
            rest = plan[2, index]
            turn = jnp.bitwise_and(128 - rest, 127)
            keep = lane < 128 - rest
            turned = []
            for t in range(tiles):
                data = extended[source, jnp.bitwise_and(tile + t, tiles - 1)].reshape(rows, 128)
                turned.append(pltpu.roll(data, turn, 1))
            for t in range(tiles):
                high, low = split(jnp.where(keep, turned[t], turned[(t + 1) % tiles]))
                left_high[slot, t, a * rows:(a + 1) * rows] = high
                left_low[slot, t, a * rows:(a + 1) * rows] = low

    def prepare(i, carry):
        position = base + i
        each, start = jnp.int32(turns[0]), jnp.int32(starts[0])
        for more, place in zip(turns[1:], starts[1:]):
            each = jnp.where(position < place * devices, each, more)
            start = jnp.where(position < place * devices, start, place)
        position = position - start * devices
        lane_group = position // each
        device = 2 * lax.rem(lane_group, devices // 2) + lane_group // (devices // 2)
        j = jnp.bitwise_xor(ids[0], device) * sum(turns) + start + lax.rem(position, each)
        q = bins[j]
        plan[0, i] = 2 * steps - offsets[j]
        plan[1, i] = lax.shift_right_logical(q, 7)
        plan[2, i] = jnp.bitwise_and(q, 127)
        return carry

    def joined(ref, extent):
        return jnp.concatenate([ref[t, :extent] for t in range(tiles)], 1)

    def multiply(block, slot):
        place = pl.ds(pl.multiple_of(block * (group * rows), group * rows), group * rows)
        left = (joined(left_high.at[slot], group * rows), joined(left_low.at[slot], group * rows))
        count = sums.shape[1]
        product = dot3(left, (joined(right_high, count), joined(right_low, count)), nt_dims)
        sums[place] = sums[place] + product

    @pl.when(k == 0)
    def _():
        lax.fori_loop(0, alphas, prepare, 0)
        for copy in pieces()[:spans]:
            copy.wait()
        build(0, 0, 0)

    def pair(i, carry):
        build(k, 2 * i + 1, 1)
        multiply(2 * i, 0)
        wrap = 2 * i + 2 == blocks
        build(jnp.where(wrap, jnp.minimum(k + 1, steps - 1), k), jnp.where(wrap, 0, 2 * i + 2), 0)
        multiply(2 * i + 1, 1)
        return carry

    lax.fori_loop(0, blocks // 2, pair, 0)

    @pl.when(k == steps - 1)
    def _():
        count = outs[0].shape[3]
        extent = outs[0].shape[0]
        if final:
            pieces()[spans].wait()

        for piece, out in enumerate(outs):

            def finish(j, carry):
                position = piece * extent + j
                cross = sums[pl.ds(pl.multiple_of(position * rows, rows), rows)]
                real = cross[:sensors, :count] + cross[sensors:, count:]
                imag = cross[sensors:, :count] - cross[:sensors, count:]
                if final:
                    real = (real + refs[10][position, 0]) * factor
                    imag = (imag + refs[10][position, 1]) * factor
                out[j, 0] = real
                out[j, 1] = imag
                return carry

            lax.fori_loop(0, extent, finish, 0, unroll=4)


def gram_sums(ids, bins, offsets, window, columns, before, turns, turn, devices, factor):
    half, tiles, _, sensors, _ = window[0].shape
    peers = len(columns)
    parts = len(columns[0])
    spans = len(window)
    final = before is not None
    outs = 2 if final else 1
    alphas = turns[turn] * devices if final else bins.shape[0]
    count = peers * sensors
    rows = 2 * sensors
    group = max(g for g in range(1, 1024 // rows + 1) if alphas % (2 * g) == 0)
    anywhere = pl.BlockSpec(memory_space=pl.ANY)
    shape = (alphas // outs, 2, sensors, count)
    return pl.pallas_call(
        functools.partial(
            gram_body, spans=spans, parts=parts, peers=peers, devices=devices, turns=turns, turn=turn, final=final, factor=factor, group=group
        ),
        grid_spec=pltpu.PrefetchScalarGridSpec(
            num_scalar_prefetch=3,
            grid=(half,),
            in_specs=[anywhere] * (spans + parts * peers + outs - 1),
            out_specs=[pl.BlockSpec(shape, lambda k, *_: (0, 0, 0, 0))] * outs,
            scratch_shapes=[
                pltpu.VMEM((3 * half, tiles, 2, sensors, 128), f32),
                pltpu.VMEM((2, peers, tiles, 2, sensors, 128), f32),
                pltpu.VMEM((2, tiles, group * rows + 16, 128), bf16),
                pltpu.VMEM((2, tiles, group * rows + 16, 128), bf16),
                pltpu.VMEM((tiles, 2 * count + 16, 128), bf16),
                pltpu.VMEM((tiles, 2 * count + 16, 128), bf16),
                pltpu.VMEM((alphas * rows, 2 * count), f32),
                pltpu.SMEM((3, alphas), jnp.int32),
                pltpu.SemaphoreType.DMA((spans + 1,)),
                pltpu.SemaphoreType.DMA((2, peers)),
            ]
            + [pltpu.VMEM((alphas, 2, sensors, count), f32)] * (outs - 1),
        ),
        out_shape=[jax.ShapeDtypeStruct(shape, f32)] * outs,
        cost_estimate=pl.CostEstimate(
            flops=6 * half * tiles * 128 * alphas * rows * 2 * count, transcendentals=0, bytes_accessed=8 << 20
        ),
        name="gram",
    )(ids, bins, offsets, *window, *[part for group in columns for part in group], *([before] if final else []))


def on_device(samples, bins, offsets):
    chan_count = lax.axis_size("chan")
    peers = lax.axis_size("sensor")
    channels = samples.shape[3]
    ids = jnp.stack([lax.axis_index("chan"), lax.axis_index("sensor")]).astype(jnp.int32)
    pieces = demodulate(samples, chan_count)
    received = []
    for side in range(2):
        received.append(lax.all_to_all(pieces[side], "chan", split_axis=0, concat_axis=0, tiled=True))
    route = [(i, (i + 1) % chan_count) for i in range(chan_count)]
    upper_whole, *uppers = whitened(received[1], 2)
    upper_rim = lax.ppermute(upper_whole, "chan", route)
    columns = [{0: part} for part in uppers]
    single = [r for r in range(1, peers) if r & (r - 1) == 0]
    for i, gathered in enumerate(columns):
        for r in single if i else single[::-1]:
            gathered[r] = swap(gathered[0], "sensor", r)
    for i, gathered in enumerate(columns):
        for r in range(1, peers):
            if r not in single:
                bits = [b for b in single if r & b]
                bit = bits[0] if i else bits[-1]
                gathered[r] = swap(gathered[r ^ bit], "sensor", bit)
    upper_columns = [[gathered[r] for gathered in columns] for r in range(peers)]
    (lower,) = whitened(received[0], 0)
    lower_columns = [[lower]] + [[swap(lower, "sensor", r)] for r in range(1, peers)]
    lower_rim = lax.ppermute(lower, "chan", route)
    factor = 1.0 / math.sqrt(channels * samples.shape[2] * chan_count)
    share = bins.shape[0] // chan_count
    turns = (share - share // 4, share // 4)
    upper_window = [upper_rim, lower] + uppers
    lower_window = [lower_rim, upper_rim, lower]
    scan = functools.partial(gram_sums, ids, bins, offsets, devices=chan_count, factor=factor)
    upper = scan(upper_window, upper_columns, None, turns, 0)[0]
    results = []
    for side in range(2):
        same, other = scan(lower_window, lower_columns, upper, turns, side)
        near = swap(other, "chan", 1)
        each = same.shape[0] // (chan_count // 2)
        total = None
        for q in range(chan_count // 2 - 1, -1, -1):
            place = slice(q * each, (q + 1) * each)
            both = same[place] + near[place]
            if q:
                both = swap(both, "chan", 2 * q)
            total = both if total is None else total + both
        results.append(total)
    return jnp.concatenate(results, 0)


def solution(mesh):
    return jax.shard_map(
        on_device,
        mesh=mesh,
        in_specs=(P(None, "sensor", "chan", None), P(), P()),
        out_specs=P("chan", None, "sensor", None),
        check_vma=False,
    )
```
